128 devices in a mesh: data: 1, expert: 128 (over z, y, x, core).
Axes of the slice: x: 4, y: 4, z: 4, core: 2. Of those that a mesh axis runs over, the one named last changes fastest.
Arguments:
- x_tok: bfloat16 [8192, 2048], P(('data', 'expert'))
- topk_idx: int32 [8192, 8], P(('data', 'expert'))
- topk_w: float32 [8192, 8], P(('data', 'expert'))
- w_up: bfloat16 [128, 2048, 768], P('expert')
- w_down: bfloat16 [128, 768, 2048], P('expert')
Outputs:
- output: bfloat16 [8192, 2048], P(('data', 'expert'))
All inputs are finite; a program needn't handle non-finite values.
Results may differ from the reference program's by a relative error of at most 0.00124.
Values are sent between devices in bfloat16 or wider.
A program may use at most 1 GiB of HBM per device.

```python
import jax
import jax.numpy as jnp
from jax import lax

D_MODEL = 2048
D_FF = 768
EXPERTS = 128
TOP_K = 8
TOK_DEV = 64
GROUP_SIZE = 128
HOT_MUL = min(4, EXPERTS // TOP_K)
SLOT_CAP = HOT_MUL * TOK_DEV * TOP_K // EXPERTS
NUM_HOT = max(1, EXPERTS // 32)
TOKENS = GROUP_SIZE * TOK_DEV


def draw_routing(key):
    hot_key, dev_key = jax.random.split(key)
    exp_perm = jax.random.permutation(hot_key, EXPERTS)
    n_cold = EXPERTS - NUM_HOT
    cold_total = TOK_DEV * TOP_K - NUM_HOT * SLOT_CAP
    base_count = cold_total // n_cold
    extra_count = cold_total - base_count * n_cold

    def one_device(dev_seed):
        shift_key, order_key, perm_key = jax.random.split(dev_seed, 3)
        shifts = jax.random.randint(shift_key, (n_cold // 2,), 0, base_count // 2 + 1)
        count_shift = jnp.concatenate([jnp.stack([shifts, -shifts], axis=1).reshape(-1), jnp.zeros((n_cold % 2,), jnp.int32)])
        cold_counts = base_count + (jnp.arange(n_cold) < extra_count).astype(jnp.int32) + count_shift
        counts = jnp.concatenate([jnp.full((NUM_HOT,), SLOT_CAP, jnp.int32), cold_counts])
        visit_order = jax.random.permutation(order_key, EXPERTS)
        run_ends = jnp.cumsum(counts[visit_order])
        run_index = jnp.searchsorted(run_ends, jnp.arange(TOK_DEV * TOP_K), side='right')
        pair_seq = exp_perm[visit_order][run_index]
        choice = pair_seq.reshape(TOP_K, TOK_DEV).T
        return choice[jax.random.permutation(perm_key, TOK_DEV)]

    dev_keys = jax.random.split(dev_key, GROUP_SIZE)
    return jax.vmap(one_device)(dev_keys).reshape(TOKENS, TOP_K).astype(jnp.int32)


def setup_inputs(seed: int = 0, part: int = 0) -> dict:
    part_key = jax.random.fold_in(jax.random.key(seed), part)
    route_key, gate_key, tok_key = jax.random.split(part_key, 3)
    up_key, down_key = jax.random.split(jax.random.key(seed + 1))
    x_tok = jax.random.normal(tok_key, (TOKENS, D_MODEL), jnp.float32).astype(jnp.bfloat16)
    topk_idx = draw_routing(route_key)
    topk_w = jax.random.uniform(gate_key, (TOKENS, TOP_K), jnp.float32, 0.1, 1.0)
    w_up = (jax.random.normal(up_key, (EXPERTS, D_MODEL, D_FF), jnp.float32) * D_MODEL ** -0.5).astype(jnp.bfloat16)
    w_down = (jax.random.normal(down_key, (EXPERTS, D_FF, D_MODEL), jnp.float32) * D_FF ** -0.5).astype(jnp.bfloat16)
    return {'x_tok': x_tok, 'topk_idx': topk_idx, 'topk_w': topk_w, 'w_up': w_up, 'w_down': w_down}


def reference(x_tok, topk_idx, topk_w, w_up, w_down):
    pair_exp = topk_idx.reshape(-1)
    n_pairs = TOKENS * TOP_K
    group_cap = GROUP_SIZE * SLOT_CAP
    sort_order = jnp.argsort(pair_exp, stable=True)
    pair_rank = jnp.argsort(sort_order, stable=True)
    counts = jnp.bincount(pair_exp, length=EXPERTS)
    starts = jnp.cumsum(counts) - counts
    slot_src = jnp.minimum(starts[:, None] + jnp.arange(group_cap)[None, :], n_pairs - 1)
    slot_tok = sort_order[slot_src] // TOP_K

    def expert_rows(operands):
        tok_ids, up_mat, down_mat = operands
        tok_rows = x_tok[tok_ids]
        hidden = jnp.dot(tok_rows, up_mat, preferred_element_type=jnp.float32)
        hidden = jax.nn.gelu(hidden, approximate=True).astype(jnp.bfloat16)
        return jnp.dot(hidden, down_mat, preferred_element_type=jnp.float32).astype(jnp.bfloat16)

    slot_out = lax.map(expert_rows, (slot_tok, w_up, w_down)).reshape(EXPERTS * group_cap, D_MODEL)
    pair_slot = pair_exp * group_cap + pair_rank - starts[pair_exp]
    pair_out = slot_out[pair_slot].reshape(TOKENS, TOP_K, D_MODEL)
    y_tok = jnp.sum(topk_w[:, :, None] * pair_out.astype(jnp.float32), axis=1)
    return y_tok.astype(jnp.bfloat16)
```

```python
import jax
import jax.numpy as jnp
from jax import lax
from jax.experimental import pallas as pl
from jax.experimental.pallas import tpu as pltpu
from jax.sharding import PartitionSpec as P

AXIS = 'expert'
LANES = 128
SLOTS = 11
TILE = 256


def route_kernel(idx_ref, pos_ref, place_ref, num_ref, cnt_ref, all_ref, send_sem, recv_sem):
    n_dev = all_ref.shape[0]
    tok_dev, top_k = idx_ref.shape
    me = lax.axis_index(AXIS)
    core = lax.rem(me, 2)
    expert = idx_ref[...]
    lane = lax.broadcasted_iota(jnp.int32, (tok_dev, n_dev), 1)
    hits = [expert[:, j:j + 1] == lane for j in range(top_k)]
    chosen = sum(h.astype(jnp.float32) for h in hits)
    counts = jnp.sum(chosen, axis=0, keepdims=True)
    cnt_ref[...] = counts.astype(jnp.int32)

    def send(k, carry):
        to = lax.rem(me + k, n_dev)
        pltpu.make_async_remote_copy(
            src_ref=cnt_ref, dst_ref=all_ref.at[me], send_sem=send_sem, recv_sem=recv_sem,
            device_id={AXIS: to}, device_id_type=pl.DeviceIdType.MESH).start()
        return carry

    lax.fori_loop(1, n_dev, send, 0)

    t_row = lax.broadcasted_iota(jnp.int32, (tok_dev, tok_dev), 0)
    t_col = lax.broadcasted_iota(jnp.int32, (tok_dev, tok_dev), 1)
    earlier = (t_col < t_row).astype(jnp.bfloat16)
    rank = jnp.dot(earlier, chosen.astype(jnp.bfloat16), preferred_element_type=jnp.float32)
    d_row = lax.broadcasted_iota(jnp.int32, (n_dev, n_dev), 0)
    d_col = lax.broadcasted_iota(jnp.int32, (n_dev, n_dev), 1)
    first_of_chip = ((d_row + 1 == d_col) & (lax.rem(d_col, 2) == 1)).astype(jnp.bfloat16)
    counts8 = jnp.broadcast_to(counts, (8, n_dev)).astype(jnp.bfloat16)
    ahead = jnp.dot(counts8, first_of_chip, preferred_element_type=jnp.float32)[:1].astype(jnp.int32)
    base = lax.broadcasted_iota(jnp.int32, (1, n_dev), 1) // 2 * (2 * SLOTS) + ahead
    slot = rank + base.astype(jnp.float32)
    slots = [jnp.sum(jnp.where(h, slot, 0.0), axis=1, keepdims=True) for h in hits]
    pos_ref[...] = jnp.concatenate(slots, axis=1).astype(jnp.int32)

    pltpu.make_async_copy(all_ref.at[pl.ds(0, n_dev - 1)], all_ref.at[pl.ds(0, n_dev - 1)], send_sem).wait()
    pltpu.make_async_copy(all_ref.at[pl.ds(0, n_dev - 1)], all_ref.at[pl.ds(0, n_dev - 1)], recv_sem).wait()

    everyone = all_ref[...].reshape(n_dev, n_dev)
    everyone = jnp.where(d_row == me, counts.astype(jnp.int32), everyone).astype(jnp.float32)
    pair_sum = ((d_row // 2 == d_col // 2)).astype(jnp.bfloat16)
    pooled = jnp.dot(everyone.astype(jnp.bfloat16), pair_sum, preferred_element_type=jnp.float32)
    peak = jnp.max(jnp.max(pooled, axis=0, keepdims=True), axis=1, keepdims=True)
    low = me - core
    n_low = jnp.sum(jnp.where(d_col == low, everyone, 0.0), axis=1, keepdims=True)
    n_both = n_low + jnp.sum(jnp.where(d_col == low + 1, everyone, 0.0), axis=1, keepdims=True)
    start = (core * SLOTS).astype(jnp.float32)
    here_low = jnp.clip(n_low - start, 0.0, SLOTS)
    here_both = jnp.clip(n_both - start, 0.0, SLOTS)
    here_high = here_both - here_low
    column = lax.broadcasted_iota(jnp.int32, (n_dev, LANES), 1)
    pair = jnp.where(column == 0, here_low, jnp.where(column == 1, here_high, 0.0)).astype(jnp.bfloat16)
    before = jnp.dot((d_col < d_row).astype(jnp.bfloat16), pair, preferred_element_type=jnp.float32)
    total_low = jnp.sum(here_low, axis=0, keepdims=True)
    total_high = jnp.sum(here_high, axis=0, keepdims=True)
    tiles_low = ((total_low.astype(jnp.int32) + TILE - 1) // TILE).astype(jnp.float32)
    tiles_high = ((total_high.astype(jnp.int32) + TILE - 1) // TILE).astype(jnp.float32)
    i = column.astype(jnp.float32)
    place = jnp.where(i < here_low, before[:, :1] + i, tiles_low * TILE + before[:, 1:2] + i - here_low)
    spare = float(spare_row(n_dev))
    place = jnp.where(i < here_both, place, spare).astype(jnp.int32)
    place_ref[...] = place[:, :SLOTS]
    who = lax.broadcasted_iota(jnp.int32, (1, n_dev), 1)
    num = jnp.where(who == 0, tiles_low, jnp.where(who == 1, tiles_low + tiles_high, peak))
    num_ref[...] = num.astype(jnp.int32)[0]


def spare_row(n_dev):
    return (pl.cdiv(n_dev * SLOTS, TILE) + 1) * TILE


def gather_kernel(pos_ref, x_ref, out_ref, rows_ref):
    tok_dev, top_k = pos_ref.shape
    rows_ref[...] = x_ref[...].reshape(rows_ref.shape)

    def body(t, carry):
        row = rows_ref[t]
        for j in range(top_k):
            out_ref[pos_ref[t, j]] = row
        return carry

    lax.fori_loop(0, tok_dev, body, 0, unroll=2)


def combine_kernel(pos_ref, gate_ref, back_ref, y_ref, acc_ref):
    tok_dev, top_k = pos_ref.shape

    def body(t, carry):
        total = gate_ref[t, 0] * back_ref[pos_ref[t, 0]].astype(jnp.float32)
        for j in range(1, top_k):
            total += gate_ref[t, j] * back_ref[pos_ref[t, j]].astype(jnp.float32)
        acc_ref[t] = total.astype(jnp.bfloat16)
        return carry

    lax.fori_loop(0, tok_dev, body, 0, unroll=2)
    y_ref[...] = acc_ref[...].reshape(y_ref.shape)


def expert_kernel(place_ref, num_ref, x_ref, up_low, down_low, up_high, down_high, out_ref, rows_ref):
    n_src = place_ref.shape[0]

    def take(s, carry):
        for i in range(SLOTS):
            p = place_ref[s, i]
            rows_ref[p // TILE, p % TILE] = x_ref[s * SLOTS + i]
        return carry

    lax.fori_loop(0, n_src, take, 0)

    def run(up_ref, down_ref):
        def tile(i, carry):
            rows = rows_ref[i].reshape(TILE, -1)
            hidden = jnp.dot(rows, up_ref[0], preferred_element_type=jnp.float32)
            hidden = jax.nn.gelu(hidden, approximate=True).astype(jnp.bfloat16)
            out = jnp.dot(hidden, down_ref[0], preferred_element_type=jnp.float32).astype(jnp.bfloat16)
            rows_ref[i] = out.reshape(rows_ref.shape[1:])
            return carry
        return tile

    lax.fori_loop(0, num_ref[0], run(up_low, down_low), 0)
    lax.fori_loop(num_ref[0], num_ref[1], run(up_high, down_high), 0)

    def give(s, carry):
        for i in range(SLOTS):
            p = place_ref[s, i]
            out_ref[s * SLOTS + i] = rows_ref[p // TILE, p % TILE]
        return carry

    lax.fori_loop(0, n_src, give, 0)


def slots_per_expert(x_loc, idx_loc, gate_loc, up_loc, down_loc, n_dev, slot_cap):
    tok_dev, d_model = x_loc.shape
    top_k = idx_loc.shape[1]
    pair_exp = idx_loc.reshape(-1)
    chosen = (idx_loc[:, :, None] == jnp.arange(n_dev)[None, None, :]).any(axis=1)
    rank = jnp.cumsum(chosen.astype(jnp.int32), axis=0) - 1
    pair_rank = jnp.take_along_axis(rank, idx_loc, axis=1).reshape(-1)
    pair_slot = pair_exp * slot_cap + pair_rank
    slot_tok = jnp.zeros((n_dev * slot_cap,), jnp.int32).at[pair_slot].set(jnp.arange(tok_dev * top_k) // top_k)
    send = jnp.take(x_loc, slot_tok, axis=0)
    recv = lax.all_to_all(send, AXIS, 0, 0, tiled=True)
    hidden = jnp.dot(recv, up_loc[0], preferred_element_type=jnp.float32)
    hidden = jax.nn.gelu(hidden, approximate=True).astype(jnp.bfloat16)
    out = jnp.dot(hidden, down_loc[0], preferred_element_type=jnp.float32).astype(jnp.bfloat16)
    back = lax.all_to_all(out, AXIS, 0, 0, tiled=True)
    rows = jnp.take(back, pair_slot, axis=0).reshape(tok_dev, top_k, d_model)
    return jnp.sum(gate_loc[:, :, None] * rows.astype(jnp.float32), axis=1).astype(jnp.bfloat16)


def solution(mesh):
    n_dev = mesh.shape[AXIS]
    swap = [(i, i ^ 1) for i in range(n_dev)]

    def local_moe(x_loc, idx_loc, gate_loc, up_loc, down_loc):
        tok_dev, d_model = x_loc.shape
        top_k = idx_loc.shape[1]
        sub = d_model // LANES
        cap = min(4, n_dev // top_k) * tok_dev * top_k // n_dev
        vmem = pl.BlockSpec(memory_space=pltpu.VMEM)
        smem = pl.BlockSpec(memory_space=pltpu.SMEM)
        pos, place, num = pl.pallas_call(
            route_kernel,
            out_shape=[jax.ShapeDtypeStruct((tok_dev, top_k), jnp.int32), jax.ShapeDtypeStruct((n_dev, SLOTS), jnp.int32),
                       jax.ShapeDtypeStruct((n_dev,), jnp.int32)],
            in_specs=[vmem], out_specs=[vmem] * 3,
            scratch_shapes=[pltpu.VMEM((1, n_dev), jnp.int32), pltpu.VMEM((n_dev, 1, n_dev), jnp.int32),
                            pltpu.SemaphoreType.DMA, pltpu.SemaphoreType.DMA],
            compiler_params=pltpu.CompilerParams(has_side_effects=True), name='route')(idx_loc)
        rows = jax.ShapeDtypeStruct((n_dev * SLOTS, sub, LANES), jnp.bfloat16)

        def pooled():
            up_other = lax.ppermute(up_loc, AXIS, swap)
            down_other = lax.ppermute(down_loc, AXIS, swap)
            send = pl.pallas_call(
                gather_kernel, out_shape=rows, in_specs=[smem, vmem], out_specs=vmem,
                scratch_shapes=[pltpu.VMEM((tok_dev, sub, LANES), jnp.bfloat16)], name='gather')(pos, x_loc)
            recv = lax.all_to_all(send, AXIS, 0, 0, tiled=True)
            odd = lax.rem(lax.axis_index(AXIS), 2) == 1
            own = (up_loc, down_loc)
            other = (up_other, down_other)

            def experts(low, high):
                return pl.pallas_call(
                    expert_kernel, out_shape=rows, in_specs=[smem, smem] + [vmem] * 5, out_specs=vmem,
                    scratch_shapes=[pltpu.VMEM((spare_row(n_dev) // TILE + 1, TILE, sub, LANES), jnp.bfloat16)],
                    compiler_params=pltpu.CompilerParams(vmem_limit_bytes=56 * 2**20), name='experts')(
                        place, num, recv, *low, *high)

            out = lax.cond(odd, lambda: experts(other, own), lambda: experts(own, other))
            back = lax.all_to_all(out, AXIS, 0, 0, tiled=True)
            return pl.pallas_call(
                combine_kernel, out_shape=jax.ShapeDtypeStruct((tok_dev, d_model), jnp.bfloat16),
                in_specs=[smem, smem, vmem], out_specs=vmem,
                scratch_shapes=[pltpu.VMEM((tok_dev, sub, LANES), jnp.bfloat16)], name='combine')(pos, gate_loc, back)

        def general():
            return slots_per_expert(x_loc, idx_loc, gate_loc, up_loc, down_loc, n_dev, cap)

        return lax.cond(num[2] <= 2 * SLOTS, pooled, general)

    tok_spec = P(('data', AXIS), None)
    w_spec = P(AXIS, None, None)
    return jax.shard_map(local_moe, mesh=mesh, in_specs=(tok_spec, tok_spec, tok_spec, w_spec, w_spec), out_specs=tok_spec, check_vma=False)
```

```python
import functools

import jax
import jax.numpy as jnp
from jax import lax
from jax.experimental import pallas as pl
from jax.experimental.pallas import tpu as pltpu
from jax.sharding import PartitionSpec as P

AXIS = 'expert'
LANES = 128
SLOT_CAP = 16
CHUNKS = (6, 5)
SLOTS = sum(CHUNKS)
REST = SLOT_CAP - SLOTS
TILE = 256
LINE = 8


def tiles_for(slots, n_dev):
    return -(-n_dev * slots // TILE) + 1


def route_kernel(idx_ref, pos_ref, *refs):
    place_refs = refs[:len(CHUNKS) + 1]
    num_ref, all_ref, send_sem, recv_sem = refs[len(CHUNKS) + 1:]
    n_dev = all_ref.shape[0]
    n_lines = n_dev // LINE
    tok_dev, top_k = idx_ref.shape
    me = lax.axis_index(AXIS)
    core = lax.rem(me, 2)
    line, here = me // LINE, lax.rem(me, LINE)
    expert = idx_ref[...]
    lane = lax.broadcasted_iota(jnp.int32, (tok_dev, n_dev), 1)
    hits = [expert[:, j:j + 1] == lane for j in range(top_k)]
    chosen = sum(h.astype(jnp.float32) for h in hits)
    counts = jnp.sum(chosen, axis=0, keepdims=True)
    all_ref[me] = counts.astype(jnp.int32)

    beside = [line * LINE + lax.rem(here + k, LINE) for k in range(1, LINE)]
    across = [lax.rem(line + k, n_lines) * LINE + here for k in range(1, n_lines)]
    barrier = pltpu.get_barrier_semaphore()
    for to in beside + across:
        pl.semaphore_signal(barrier, inc=1, device_id={AXIS: to}, device_id_type=pl.DeviceIdType.MESH)
    pl.semaphore_wait(barrier, len(beside) + len(across))

    def send(rows, to, phase):
        pltpu.make_async_remote_copy(
            src_ref=all_ref.at[rows], dst_ref=all_ref.at[rows], send_sem=send_sem.at[phase], recv_sem=recv_sem.at[phase],
            device_id={AXIS: to}, device_id_type=pl.DeviceIdType.MESH).start()

    def settle(sem, rows):
        pltpu.make_async_copy(all_ref.at[pl.ds(0, rows)], all_ref.at[pl.ds(0, rows)], sem).wait()

    for to in beside:
        send(pl.ds(me, 1), to, 0)

    t_row = lax.broadcasted_iota(jnp.int32, (tok_dev, tok_dev), 0)
    t_col = lax.broadcasted_iota(jnp.int32, (tok_dev, tok_dev), 1)
    earlier = (t_col < t_row).astype(jnp.bfloat16)
    rank = jnp.dot(earlier, chosen.astype(jnp.bfloat16), preferred_element_type=jnp.float32)
    d_row = lax.broadcasted_iota(jnp.int32, (n_dev, n_dev), 0)
    d_col = lax.broadcasted_iota(jnp.int32, (n_dev, n_dev), 1)
    first_of_chip = ((d_row + 1 == d_col) & (lax.rem(d_col, 2) == 1)).astype(jnp.bfloat16)
    counts8 = jnp.broadcast_to(counts, (8, n_dev)).astype(jnp.bfloat16)
    ahead = jnp.dot(counts8, first_of_chip, preferred_element_type=jnp.float32)[:1]
    slot = rank + ahead

    settle(recv_sem.at[0], LINE - 1)
    for to in across:
        send(pl.ds(line * LINE, LINE), to, 1)

    p = jnp.concatenate([jnp.sum(jnp.where(h, slot, 0.0), axis=1, keepdims=True) for h in hits], axis=1).astype(jnp.int32)
    chip0 = expert - lax.rem(expert, 2)
    second = (p >= SLOTS).astype(jnp.int32)
    i = p - second * SLOTS
    pos = (chip0 + second) * CHUNKS[0] + i
    pos = jnp.where(i >= CHUNKS[0], n_dev * CHUNKS[0] + (chip0 + second) * CHUNKS[1] + i - CHUNKS[0], pos)
    i = p - 2 * SLOTS
    second = (i >= REST).astype(jnp.int32)
    late = n_dev * SLOTS + (chip0 + second) * REST + i - second * REST
    pos_ref[...] = jnp.where(p >= 2 * SLOTS, late, pos)

    settle(send_sem.at[0], LINE - 1)
    settle(send_sem.at[1], n_dev - LINE)
    settle(recv_sem.at[1], n_dev - LINE)

    everyone = all_ref[...].reshape(n_dev, n_dev).astype(jnp.float32)
    pair_sum = ((d_row // 2 == d_col // 2)).astype(jnp.bfloat16)
    pooled = jnp.dot(everyone.astype(jnp.bfloat16), pair_sum, preferred_element_type=jnp.float32)
    peak = jnp.max(jnp.max(pooled, axis=0, keepdims=True), axis=1, keepdims=True)
    low = me - core
    n_low = jnp.sum(jnp.where(d_col == low, everyone, 0.0), axis=1, keepdims=True)
    n_both = n_low + jnp.sum(jnp.where(d_col == low + 1, everyone, 0.0), axis=1, keepdims=True)
    column = lax.broadcasted_iota(jnp.int32, (n_dev, LANES), 1)
    windows = [(core * SLOTS, CHUNKS[0]), (core * SLOTS + CHUNKS[0], CHUNKS[1]), (2 * SLOTS + core * REST, REST)]
    spans = []
    packed = jnp.zeros((n_dev, LANES), jnp.float32)
    for k, (start, size) in enumerate(windows):
        start = start.astype(jnp.float32)
        here_low = jnp.clip(n_low - start, 0.0, size)
        here_both = jnp.clip(n_both - start, 0.0, size)
        spans.append((here_low, here_both))
        packed = jnp.where(column == 2 * k, here_low, jnp.where(column == 2 * k + 1, here_both - here_low, packed))
    before = jnp.dot((d_col < d_row).astype(jnp.bfloat16), packed.astype(jnp.bfloat16), preferred_element_type=jnp.float32)
    totals = jnp.sum(packed, axis=0, keepdims=True)
    tiles = (totals.astype(jnp.int32) + TILE - 1) // TILE
    tiles = tiles.astype(jnp.float32)
    who = lax.broadcasted_iota(jnp.int32, (1, n_dev), 1)
    num = jnp.where(who == 2 * len(windows), peak, 0.0)
    is_high = core.astype(jnp.float32)
    lanes = column.astype(jnp.float32)
    for k, (start, size) in enumerate(windows):
        here_low, here_both = spans[k]
        t_low, t_high = tiles[:, 2 * k:2 * k + 1], tiles[:, 2 * k + 1:2 * k + 2]
        at_low = is_high * t_high * TILE + before[:, 2 * k:2 * k + 1] + lanes
        at_high = (1.0 - is_high) * t_low * TILE + before[:, 2 * k + 1:2 * k + 2] + lanes - here_low
        place = jnp.where(lanes < here_low, at_low, at_high)
        place = jnp.where(lanes < here_both, place, float(tiles_for(size, n_dev) * TILE)).astype(jnp.int32)
        place_refs[k][...] = place[:, :size]
        own = is_high * t_high + (1.0 - is_high) * t_low
        num = jnp.where(who == 2 * k, own, jnp.where(who == 2 * k + 1, t_low + t_high, num))
    num_ref[...] = num.astype(jnp.int32)[0]


def pack_kernel(first, counts, pos_ref, x_ref, *refs):
    out_refs, (rows_ref, slots_ref, sems) = refs[:len(counts)], refs[len(counts):]
    tok_dev, top_k = pos_ref.shape
    rows_ref[...] = x_ref[...].reshape(rows_ref.shape)
    spare = sum(counts)

    def body(t, carry):
        row = rows_ref[t]
        for j in range(top_k):
            at = pos_ref[t, j] - first
            at = jnp.where((at >= 0) & (at < spare), at, spare)
            slots_ref[at] = row
        return carry

    lax.fori_loop(0, tok_dev, body, 0, unroll=2)
    copies, start = [], 0
    for k, count in enumerate(counts):
        copies.append(pltpu.make_async_copy(slots_ref.at[pl.ds(start, count)], out_refs[k], sems.at[k]))
        copies[-1].start()
        start += count
    for copy in copies:
        copy.wait()


def combine_kernel(first, counts, pos_ref, gate_ref, acc_in_ref, *refs):
    back_refs, (y_ref, acc_ref, slots_ref, round_ref, sems) = refs[:len(counts)], refs[len(counts):]
    tok_dev, top_k = pos_ref.shape
    spare = sum(counts)
    copies, start = [], 0
    for k, count in enumerate(counts):
        copies.append(pltpu.make_async_copy(back_refs[k], slots_ref.at[pl.ds(start, count)], sems.at[k]))
        copies[-1].start()
        start += count
    slots_ref[spare] = jnp.zeros(slots_ref.shape[1:], slots_ref.dtype)
    for copy in copies:
        copy.wait()

    def body(t, carry):
        total = jnp.zeros(slots_ref.shape[1:], jnp.float32) if acc_in_ref is None else acc_in_ref[t]
        for j in range(top_k):
            at = pos_ref[t, j] - first
            at = jnp.where((at >= 0) & (at < spare), at, spare)
            total += gate_ref[t, j] * slots_ref[at].astype(jnp.float32)
        acc_ref[t] = total
        round_ref[t] = total.astype(jnp.bfloat16)
        return carry

    lax.fori_loop(0, tok_dev, body, 0, unroll=2)
    y_ref[...] = round_ref[...].reshape(y_ref.shape)


def first_combine_kernel(first, counts, pos_ref, gate_ref, *refs):
    combine_kernel(first, counts, pos_ref, gate_ref, None, *refs)


def expert_kernel(at, place_ref, num_ref, x_ref, up_own, down_own, up_other, down_other, out_ref, rows_ref):
    n_src, slots = place_ref.shape

    def take(s, carry):
        for i in range(slots):
            p = place_ref[s, i]
            rows_ref[p // TILE, p % TILE] = x_ref[s * slots + i]
        return carry

    lax.fori_loop(0, n_src, take, 0)

    def run(up_ref, down_ref):
        def tile(i, carry):
            rows = rows_ref[i].reshape(TILE, -1)
            hidden = jnp.dot(rows, up_ref[0], preferred_element_type=jnp.float32)
            hidden = jax.nn.gelu(hidden, approximate=True).astype(jnp.bfloat16)
            out = jnp.dot(hidden, down_ref[0], preferred_element_type=jnp.float32).astype(jnp.bfloat16)
            rows_ref[i] = out.reshape(rows_ref.shape[1:])
            return carry
        return tile

    lax.fori_loop(0, num_ref[at], run(up_own, down_own), 0)
    lax.fori_loop(num_ref[at], num_ref[at + 1], run(up_other, down_other), 0)

    def give(s, carry):
        for i in range(slots):
            p = place_ref[s, i]
            out_ref[s * slots + i] = rows_ref[p // TILE, p % TILE]
        return carry

    lax.fori_loop(0, n_src, give, 0)


def solution(mesh):
    n_dev = mesh.shape[AXIS]
    swap = [(i, i ^ 1) for i in range(n_dev)]

    def local_moe(x_loc, idx_loc, gate_loc, up_loc, down_loc):
        tok_dev, d_model = x_loc.shape
        top_k = idx_loc.shape[1]
        d_ff = up_loc.shape[2]
        sub = d_model // LANES
        vmem = pl.BlockSpec(memory_space=pltpu.VMEM)
        smem = pl.BlockSpec(memory_space=pltpu.SMEM)
        anywhere = pl.BlockSpec(memory_space=pl.ANY)
        tile_of = lambda n, dtype=jnp.bfloat16: jax.ShapeDtypeStruct((n, sub, LANES), dtype)
        sizes = CHUNKS + (REST,)
        pos, *places, num = pl.pallas_call(
            route_kernel,
            out_shape=[jax.ShapeDtypeStruct((tok_dev, top_k), jnp.int32)]
            + [jax.ShapeDtypeStruct((n_dev, size), jnp.int32) for size in sizes] + [jax.ShapeDtypeStruct((n_dev,), jnp.int32)],
            in_specs=[vmem], out_specs=[vmem] * (len(sizes) + 2),
            scratch_shapes=[pltpu.VMEM((n_dev, 1, n_dev), jnp.int32), pltpu.SemaphoreType.DMA((2,)), pltpu.SemaphoreType.DMA((2,))],
            compiler_params=pltpu.CompilerParams(has_side_effects=True, collective_id=0), name='route')(idx_loc)
        up_other = lax.ppermute(up_loc, AXIS, swap)
        down_other = lax.ppermute(down_loc, AXIS, swap)

        def exchange(rows):
            return lax.all_to_all(rows, AXIS, 0, 0, tiled=True)

        def send_rows(first, counts):
            return pl.pallas_call(
                functools.partial(pack_kernel, first, counts), out_shape=[tile_of(c) for c in counts],
                in_specs=[smem, vmem], out_specs=[anywhere] * len(counts),
                scratch_shapes=[pltpu.VMEM((tok_dev, sub, LANES), jnp.bfloat16), pltpu.VMEM((sum(counts) + 8, sub, LANES), jnp.bfloat16),
                                pltpu.SemaphoreType.DMA((len(counts),))], name='pack')(pos, x_loc)

        def experts(k, rows):
            size = sizes[k]
            n_rows = n_dev * size
            return pl.pallas_call(
                functools.partial(expert_kernel, 2 * k), out_shape=tile_of(n_rows), in_specs=[smem, smem] + [vmem] * 5, out_specs=vmem,
                scratch_shapes=[pltpu.VMEM((tiles_for(size, n_dev) + 1, TILE, sub, LANES), jnp.bfloat16)],
                cost_estimate=pl.CostEstimate(flops=4 * n_rows * d_model * d_ff, bytes_accessed=4 * n_rows * d_model + 8 * d_model * d_ff,
                                              transcendentals=n_rows * d_ff),
                compiler_params=pltpu.CompilerParams(vmem_limit_bytes=44 * 2**20), name=f'experts{k}')(
                    places[k], num, rows, up_loc, down_loc, up_other, down_other)

        def add_up(first, counts, backs, acc):
            body = first_combine_kernel if acc is None else combine_kernel
            extra = [] if acc is None else [acc]
            return pl.pallas_call(
                functools.partial(body, first, counts),
                out_shape=[jax.ShapeDtypeStruct((tok_dev, d_model), jnp.bfloat16), tile_of(tok_dev, jnp.float32)],
                in_specs=[smem, smem] + [vmem] * len(extra) + [anywhere] * len(counts), out_specs=[vmem, vmem],
                scratch_shapes=[pltpu.VMEM((sum(counts) + 8, sub, LANES), jnp.bfloat16), pltpu.VMEM((tok_dev, sub, LANES), jnp.bfloat16),
                                pltpu.SemaphoreType.DMA((len(counts),))], name='combine')(pos, gate_loc, *extra, *backs)

        counts = tuple(n_dev * c for c in CHUNKS)
        sent = send_rows(0, counts)
        came = [exchange(rows) for rows in sent]
        back = [exchange(experts(k, rows)) for k, rows in enumerate(came)]
        y, acc = add_up(0, counts, back, None)

        def second_pass():
            first, count = sum(counts), (n_dev * REST,)
            rows = exchange(send_rows(first, count)[0])
            return add_up(first, count, [exchange(experts(len(CHUNKS), rows))], acc)[0]

        return lax.cond(num[2 * len(sizes)] <= 2 * SLOTS, lambda: y, second_pass)

    tok_spec = P(('data', AXIS), None)
    w_spec = P(AXIS, None, None)
    return jax.shard_map(local_moe, mesh=mesh, in_specs=(tok_spec, tok_spec, tok_spec, w_spec, w_spec), out_specs=tok_spec, check_vma=False)
```

```python
import jax
import jax.numpy as jnp
from jax import lax
from jax.experimental import pallas as pl
from jax.experimental.pallas import tpu as pltpu
from jax.sharding import PartitionSpec as P

AXIS = 'expert'
LANES = 128
SLOT_CAP = 16
SLOTS = 11
REST = SLOT_CAP - SLOTS
LINE = 8
PAIR = 2


def copy_rows(pos_ref, rows_ref, slots_ref, first, count):
    top_k, tok_dev = pos_ref.shape

    def body(t, carry):
        row = rows_ref[t]
        for j in range(top_k):
            at = pos_ref[j, t] - first
            at = jnp.minimum(at, count) if first == 0 else jnp.where(at < 0, count, at)
            slots_ref[at] = row
        return carry

    lax.fori_loop(0, tok_dev, body, 0, unroll=2)


def pack_kernel(idx_ref, x_ref, out_ref, pos_ref, counts_ref, rows_ref, slots_ref, pos_smem, sems):
    top_k, tok_dev = idx_ref.shape
    n_exp = counts_ref.shape[1]
    expert = lax.broadcasted_iota(jnp.int32, (n_exp, tok_dev), 0)
    hits = [idx_ref[j:j + 1, :] == expert for j in range(top_k)]
    chosen = sum(h.astype(jnp.float32) for h in hits).astype(jnp.bfloat16)
    t_row = lax.broadcasted_iota(jnp.int32, (tok_dev, tok_dev), 0)
    t_col = lax.broadcasted_iota(jnp.int32, (tok_dev, tok_dev), 1)
    rank = jnp.dot(chosen, (t_row < t_col).astype(jnp.bfloat16), preferred_element_type=jnp.float32)
    e_row = lax.broadcasted_iota(jnp.int32, (n_exp, n_exp), 0)
    e_col = lax.broadcasted_iota(jnp.int32, (n_exp, n_exp), 1)
    beside = ((e_col + 1 == e_row) & (lax.rem(e_row, 2) == 1)).astype(jnp.bfloat16)
    ahead = jnp.sum(jnp.dot(beside, chosen, preferred_element_type=jnp.float32), axis=1, keepdims=True)
    odd = lax.rem(expert, 2)
    chip0 = (expert - odd).astype(jnp.float32)
    p = jnp.where(odd == 1, 2 * SLOTS - 1 - rank, rank)
    core = (p >= SLOTS).astype(jnp.float32)
    slot = (chip0 + core) * SLOTS + p - core * SLOTS
    late = ahead + rank - 2 * SLOTS
    core = (late >= REST).astype(jnp.float32)
    late_slot = n_exp * SLOTS + (chip0 + core) * REST + late - core * REST
    slot = jnp.where((odd == 1) & (late >= 0), late_slot, slot)
    pos = jnp.concatenate([jnp.sum(jnp.where(h, slot, 0.0), axis=0, keepdims=True) for h in hits], axis=0)
    pos_ref[...] = pos.astype(jnp.int32)
    to_smem = pltpu.make_async_copy(pos_ref, pos_smem, sems.at[0])
    to_smem.start()
    counts = lax.dot_general(jnp.ones((8, tok_dev), jnp.bfloat16), chosen, (((1,), (1,)), ((), ())), preferred_element_type=jnp.float32)
    counts_ref[...] = counts[:1].astype(jnp.int32)
    rows_ref[...] = x_ref[...].reshape(rows_ref.shape)
    to_smem.wait()
    count = out_ref.shape[0]
    copy_rows(pos_smem, rows_ref, slots_ref, 0, count)
    out = pltpu.make_async_copy(slots_ref.at[pl.ds(0, count)], out_ref, sems.at[1])
    out.start()
    out.wait()


def pack_late_kernel(pos_ref, x_ref, out_ref, rows_ref, slots_ref, sems):
    count = out_ref.shape[0]
    rows_ref[...] = x_ref[...].reshape(rows_ref.shape)
    copy_rows(pos_ref, rows_ref, slots_ref, count // REST * SLOTS, count)
    out = pltpu.make_async_copy(slots_ref.at[pl.ds(0, count)], out_ref, sems.at[0])
    out.start()
    out.wait()


def route_kernel(counts_ref, low_ref, num_ref, all_ref, send_sem, recv_sem):
    n_dev = all_ref.shape[0]
    n_lines = n_dev // LINE
    me = lax.axis_index(AXIS)
    core = lax.rem(me, 2)
    line, here = me // LINE, lax.rem(me, LINE)
    all_ref[me] = counts_ref[...]
    beside = [line * LINE + lax.rem(here + k, LINE) for k in range(1, LINE)]
    across = [lax.rem(line + k, n_lines) * LINE + here for k in range(1, n_lines)]
    barrier = pltpu.get_barrier_semaphore()
    for to in beside + across:
        pl.semaphore_signal(barrier, inc=1, device_id={AXIS: to}, device_id_type=pl.DeviceIdType.MESH)
    pl.semaphore_wait(barrier, len(beside) + len(across))

    def send(rows, to, phase):
        pltpu.make_async_remote_copy(
            src_ref=all_ref.at[rows], dst_ref=all_ref.at[rows], send_sem=send_sem.at[phase], recv_sem=recv_sem.at[phase],
            device_id={AXIS: to}, device_id_type=pl.DeviceIdType.MESH).start()

    def settle(sem, rows):
        pltpu.make_async_copy(all_ref.at[pl.ds(0, rows)], all_ref.at[pl.ds(0, rows)], sem).wait()

    for to in beside:
        send(pl.ds(me, 1), to, 0)
    settle(recv_sem.at[0], LINE - 1)
    for to in across:
        send(pl.ds(line * LINE, LINE), to, 1)
    settle(send_sem.at[0], LINE - 1)
    settle(send_sem.at[1], n_dev - LINE)
    settle(recv_sem.at[1], n_dev - LINE)

    everyone = all_ref[...].reshape(n_dev, n_dev).astype(jnp.float32)
    row = lax.broadcasted_iota(jnp.int32, (n_dev, n_dev), 0)
    col = lax.broadcasted_iota(jnp.int32, (n_dev, n_dev), 1)
    pooled = jnp.dot(everyone.astype(jnp.bfloat16), (row // 2 == col // 2).astype(jnp.bfloat16), preferred_element_type=jnp.float32)
    top = lambda v: jnp.max(jnp.max(v, axis=0, keepdims=True), axis=1, keepdims=True)
    first = me - core
    low = jnp.sum(jnp.where(col == first, everyone, 0.0), axis=1, keepdims=True)
    high = jnp.sum(jnp.where(col == first + 1, everyone, 0.0), axis=1, keepdims=True)
    high = jnp.minimum(high, 2 * SLOTS - low)
    who = lax.broadcasted_iota(jnp.int32, (1, n_dev), 1)
    num = jnp.where(who == 0, top(low), jnp.where(who == 1, top(high), top(pooled)))
    num_ref[...] = num.astype(jnp.int32)[0]
    twice_row = lax.broadcasted_iota(jnp.int32, (PAIR * n_dev, n_dev), 0)
    twice_col = lax.broadcasted_iota(jnp.int32, (PAIR * n_dev, n_dev), 1)
    spread = (twice_row // PAIR == twice_col).astype(jnp.bfloat16)
    lows = jnp.broadcast_to(low, (n_dev, n_dev)).astype(jnp.bfloat16)
    low_ref[...] = jnp.dot(spread, lows, preferred_element_type=jnp.float32) - lax.rem(twice_row, PAIR).astype(jnp.float32)


def mlp(rows, up, down):
    hidden = jnp.dot(rows, up, preferred_element_type=jnp.float32)
    hidden = jax.nn.gelu(hidden, approximate=True).astype(jnp.bfloat16)
    return jnp.dot(hidden, down, preferred_element_type=jnp.float32).astype(jnp.bfloat16)


def expert_kernel(num_ref, low_ref, x_ref, up_own, down_own, up_other, down_other, out_ref, rows_ref, up_ref, down_ref, w_sems, in_sems, out_sems):
    slots = x_ref.shape[1]
    groups = pl.cdiv(slots, PAIR)
    core = lax.rem(lax.axis_index(AXIS), 2)
    loads = []
    for k, (up, down) in enumerate(((up_own, down_own), (up_other, down_other))):
        loads.append((pltpu.make_async_copy(up.at[0], up_ref.at[k], w_sems.at[k, 0]),
                      pltpu.make_async_copy(down.at[0], down_ref.at[k], w_sems.at[k, 1])))

    def move(g, size, back):
        here, there = rows_ref.at[g, :, pl.ds(0, size)], (out_ref if back else x_ref).at[:, pl.ds(g * PAIR, size)]
        return pltpu.make_async_copy(here, there, out_sems.at[g]) if back else pltpu.make_async_copy(there, here, in_sems.at[g])

    size_of = [min(PAIR, slots - g * PAIR) for g in range(groups)]
    move(0, size_of[0], False).start()
    for load in loads[0]:
        load.start()
    for g in range(1, groups):
        move(g, size_of[g], False).start()
    for load in loads[1]:
        load.start()
    for pair in loads:
        for load in pair:
            load.wait()
    n_low, n_high = num_ref[0], num_ref[1]

    def each_size(g, act):
        @pl.when(g < groups - 1)
        def _():
            act(PAIR)

        @pl.when(g == groups - 1)
        def _():
            act(size_of[-1])

    def group(g, carry):
        each_size(g, lambda size: move(g, size, False).wait())
        p = core * slots + g * PAIR
        has_low = p < n_low
        has_high = jnp.minimum(p + PAIR, (core + 1) * slots) > 2 * slots - n_high

        @pl.when(has_low != has_high)
        def _():
            k = jnp.where(has_low, core, 1 - core)
            out = mlp(rows_ref[g].reshape(PAIR * rows_ref.shape[1], -1), up_ref[k], down_ref[k])
            rows_ref[g] = out.reshape(rows_ref.shape[1:])

        @pl.when(has_low & has_high)
        def _():
            rows = rows_ref[g].reshape(PAIR * rows_ref.shape[1], -1)
            first = mlp(rows, up_ref[core], down_ref[core])
            second = mlp(rows, up_ref[1 - core], down_ref[1 - core])
            out = jnp.where(low_ref[:, :1] > p.astype(jnp.float32), first.astype(jnp.float32), second.astype(jnp.float32)).astype(jnp.bfloat16)
            rows_ref[g] = out.reshape(rows_ref.shape[1:])

        each_size(g, lambda size: move(g, size, True).start())
        return carry

    lax.fori_loop(0, groups, group, 0)
    for g in range(groups):
        move(g, size_of[g], True).wait()


def late_expert_kernel(x_ref, up_ref, down_ref, out_ref):
    def tile(i, carry):
        out_ref[i] = mlp(x_ref[i].reshape(x_ref.shape[1], -1), up_ref[0], down_ref[0]).reshape(x_ref.shape[1:])
        return carry

    lax.fori_loop(0, x_ref.shape[0], tile, 0)


def combine_kernel(pos_ref, gate_ref, back_ref, *refs):
    late_ref, (y_ref, acc_ref) = (refs[0] if len(refs) == 3 else None), refs[-2:]
    top_k, tok_dev = pos_ref.shape
    count = back_ref.shape[0]

    def body(t, carry):
        total = None
        for j in range(top_k):
            at = pos_ref[j, t]
            row = back_ref[jnp.minimum(at, count - 1)]
            if late_ref is not None:
                row = jnp.where(at < count, row, late_ref[jnp.maximum(at - count, 0)])
            term = gate_ref[j, t] * row.astype(jnp.float32)
            total = term if total is None else total + term
        acc_ref[t] = total.astype(jnp.bfloat16)
        return carry

    lax.fori_loop(0, tok_dev, body, 0, unroll=2)
    y_ref[...] = acc_ref[...].reshape(y_ref.shape)


def solution(mesh):
    n_dev = mesh.shape[AXIS]
    swap = [(i, i ^ 1) for i in range(n_dev)]

    def local_moe(x_loc, idx_loc, gate_loc, up_loc, down_loc):
        tok_dev, d_model = x_loc.shape
        top_k = idx_loc.shape[1]
        d_ff = up_loc.shape[2]
        sub = d_model // LANES
        count, late_count = n_dev * SLOTS, n_dev * REST
        vmem = pl.BlockSpec(memory_space=pltpu.VMEM)
        smem = pl.BlockSpec(memory_space=pltpu.SMEM)
        anywhere = pl.BlockSpec(memory_space=pl.ANY)
        tile_of = lambda n: jax.ShapeDtypeStruct((n, sub, LANES), jnp.bfloat16)
        dma = pltpu.SemaphoreType.DMA
        scratch = lambda *shape: pltpu.VMEM(shape + (sub, LANES), jnp.bfloat16)
        idx_t, gate_t = idx_loc.T, gate_loc.T
        up_other = lax.ppermute(up_loc, AXIS, swap)
        down_other = lax.ppermute(down_loc, AXIS, swap)

        def exchange(rows):
            return lax.all_to_all(rows, AXIS, 0, 0, tiled=True)

        sent, pos, counts = pl.pallas_call(
            pack_kernel,
            out_shape=[tile_of(count), jax.ShapeDtypeStruct((top_k, tok_dev), jnp.int32), jax.ShapeDtypeStruct((1, n_dev), jnp.int32)],
            in_specs=[vmem, vmem], out_specs=[anywhere, vmem, vmem],
            scratch_shapes=[scratch(tok_dev), scratch(count + 8), pltpu.SMEM((top_k, tok_dev), jnp.int32), dma((2,))],
            name='pack')(idx_t, x_loc)
        came = exchange(sent)
        low, num = pl.pallas_call(
            route_kernel,
            out_shape=[jax.ShapeDtypeStruct((PAIR * n_dev, n_dev), jnp.float32), jax.ShapeDtypeStruct((n_dev,), jnp.int32)],
            in_specs=[vmem], out_specs=[vmem, vmem],
            scratch_shapes=[pltpu.VMEM((n_dev, 1, n_dev), jnp.int32), dma((2,)), dma((2,))],
            cost_estimate=pl.CostEstimate(flops=10**10, bytes_accessed=10**5, transcendentals=0),
            compiler_params=pltpu.CompilerParams(has_side_effects=True, collective_id=0), name='route')(counts)
        groups = -(-SLOTS // PAIR)
        done = pl.pallas_call(
            expert_kernel, out_shape=jax.ShapeDtypeStruct((n_dev, SLOTS, sub, LANES), jnp.bfloat16),
            in_specs=[smem, vmem] + [anywhere] * 5, out_specs=pl.BlockSpec(memory_space=pltpu.HBM),
            scratch_shapes=[scratch(groups, n_dev, PAIR), pltpu.VMEM((2, d_model, d_ff), jnp.bfloat16), pltpu.VMEM((2, d_ff, d_model), jnp.bfloat16),
                            dma((2, 2)), dma((groups,)), dma((groups,))],
            cost_estimate=pl.CostEstimate(flops=4 * count * d_model * d_ff, bytes_accessed=4 * count * d_model + 8 * d_model * d_ff,
                                          transcendentals=count * d_ff),
            compiler_params=pltpu.CompilerParams(vmem_limit_bytes=44 * 2**20), name='experts')(
                num, low, came.reshape(n_dev, SLOTS, sub, LANES), up_loc, down_loc, up_other, down_other)
        back = exchange(done.reshape(count, sub, LANES))

        def combine(*backs):
            return pl.pallas_call(
                combine_kernel, out_shape=jax.ShapeDtypeStruct((tok_dev, d_model), jnp.bfloat16),
                in_specs=[smem, smem] + [vmem] * len(backs), out_specs=vmem, scratch_shapes=[scratch(tok_dev)], name='combine')(pos, gate_t, *backs)

        def second_pass():
            rows = pl.pallas_call(
                pack_late_kernel, out_shape=tile_of(late_count), in_specs=[smem, vmem], out_specs=anywhere,
                scratch_shapes=[scratch(tok_dev), scratch(late_count + 8), dma((1,))], name='pack_late')(pos, x_loc)
            odd = lax.rem(lax.axis_index(AXIS), 2) == 1
            up, down = jnp.where(odd, up_loc, up_other), jnp.where(odd, down_loc, down_other)
            out = pl.pallas_call(
                late_expert_kernel, out_shape=jax.ShapeDtypeStruct((REST, n_dev, sub, LANES), jnp.bfloat16),
                in_specs=[vmem] * 3, out_specs=vmem, name='late_experts')(exchange(rows).reshape(REST, n_dev, sub, LANES), up, down)
            return combine(back, exchange(out.reshape(late_count, sub, LANES)))

        return lax.cond(num[2] <= 2 * SLOTS, lambda: combine(back), second_pass)

    tok_spec = P(('data', AXIS), None)
    w_spec = P(AXIS, None, None)
    return jax.shard_map(local_moe, mesh=mesh, in_specs=(tok_spec, tok_spec, tok_spec, w_spec, w_spec), out_specs=tok_spec, check_vma=False)
```

```python
import jax
import jax.numpy as jnp
from jax import lax
from jax.experimental import pallas as pl
from jax.experimental.pallas import tpu as pltpu
from jax.sharding import PartitionSpec as P

AXIS = 'expert'
LANES = 128
SLOT_CAP = 16
SLOTS = 11
REST = SLOT_CAP - SLOTS
PAIR = 2
HEAD = 8
STRIDE = 256


def copy_rows(rows_ref, top_k, put):
    def body(t, carry):
        row = rows_ref[t]
        for j in range(top_k):
            put(j, t, row)
        return carry

    lax.fori_loop(0, rows_ref.shape[0], body, 0, unroll=2)


def pack_kernel(idx_ref, x_ref, out_ref, pos_ref, rows_ref, blocks_ref, at_ref, at_smem, sems):
    top_k, tok_dev = idx_ref.shape
    n_exp = out_ref.shape[0]
    sub = rows_ref.shape[1]
    expert = lax.broadcasted_iota(jnp.int32, (n_exp, tok_dev), 0)
    hits = [idx_ref[j:j + 1, :] == expert for j in range(top_k)]
    chosen = sum(h.astype(jnp.float32) for h in hits)
    t_row = lax.broadcasted_iota(jnp.int32, (tok_dev, tok_dev), 0)
    t_col = lax.broadcasted_iota(jnp.int32, (tok_dev, tok_dev), 1)
    rank = jnp.dot(chosen.astype(jnp.bfloat16), (t_row < t_col).astype(jnp.bfloat16), preferred_element_type=jnp.float32)
    counts = jnp.broadcast_to(jnp.sum(chosen, axis=1, keepdims=True), (n_exp, n_exp)).astype(jnp.bfloat16)
    e_row = lax.broadcasted_iota(jnp.int32, (n_exp, n_exp), 0)
    e_col = lax.broadcasted_iota(jnp.int32, (n_exp, n_exp), 1)
    first = e_row - lax.rem(e_row, 2)
    low = jnp.dot((e_col == first).astype(jnp.bfloat16), counts, preferred_element_type=jnp.float32)
    high = jnp.dot((e_col == first + 1).astype(jnp.bfloat16), counts, preferred_element_type=jnp.float32)
    odd = lax.rem(expert, 2)
    chip0 = (expert - odd).astype(jnp.float32)
    p = jnp.where(odd == 1, 2 * SLOTS - 1 - rank, rank)
    core = (p >= SLOTS).astype(jnp.float32)
    i = p - core * SLOTS
    late = low[:, :1] + rank - 2 * SLOTS
    is_late = (odd == 1) & (late >= 0)
    late_core = (late >= REST).astype(jnp.float32)
    slot = jnp.where(is_late, n_exp * SLOTS + (chip0 + late_core) * REST + late - late_core * REST, (chip0 + core) * SLOTS + i)
    at = jnp.where(is_late, float(n_exp * STRIDE), (chip0 + core) * STRIDE + i * sub)
    of_pair = lambda v: jnp.concatenate([jnp.sum(jnp.where(h, v, 0.0), axis=0, keepdims=True) for h in hits], axis=0).astype(jnp.int32)
    at_ref[...] = of_pair(at)
    to_smem = pltpu.make_async_copy(at_ref, at_smem, sems.at[0])
    to_smem.start()
    pos_ref[...] = of_pair(slot)
    left_over = jnp.max(jnp.max(low + high - 2 * SLOTS, axis=0, keepdims=True), axis=1, keepdims=True) > 0
    line = lax.broadcasted_iota(jnp.int32, (n_exp, HEAD, LANES), 1)
    head = jnp.where(line == 0, low[:, None, :], jnp.where(line == 1, high[:, None, :], left_over.astype(jnp.float32)[:, None, :]))
    blocks_ref[pl.ds(0, n_exp), pl.ds(SLOTS * sub, HEAD)] = head.astype(jnp.bfloat16)
    rows_ref[...] = x_ref[...].reshape(rows_ref.shape)
    to_smem.wait()

    def put(j, t, row):
        at = at_smem[j, t]
        blocks_ref[at // STRIDE, pl.ds(pl.multiple_of(at % STRIDE, sub), sub)] = row

    copy_rows(rows_ref, top_k, put)
    out = pltpu.make_async_copy(blocks_ref.at[pl.ds(0, n_exp)], out_ref, sems.at[1])
    out.start()
    out.wait()


def pack_late_kernel(pos_ref, x_ref, out_ref, rows_ref, slots_ref, sems):
    count = out_ref.shape[0]
    rows_ref[...] = x_ref[...].reshape(rows_ref.shape)

    def put(j, t, row):
        at = pos_ref[j, t] - count // REST * SLOTS
        slots_ref[jnp.where(at < 0, count, at)] = row

    copy_rows(rows_ref, pos_ref.shape[0], put)
    out = pltpu.make_async_copy(slots_ref.at[pl.ds(0, count)], out_ref, sems.at[0])
    out.start()
    out.wait()


def mlp(rows, up, down):
    hidden = jnp.dot(rows, up, preferred_element_type=jnp.float32)
    hidden = jax.nn.gelu(hidden, approximate=True).astype(jnp.bfloat16)
    return jnp.dot(hidden, down, preferred_element_type=jnp.float32).astype(jnp.bfloat16)


def expert_kernel(x_ref, up_own, down_own, up_other, down_other, out_ref, left_ref, rows_ref, head_ref, up_ref, down_ref, ready_ref,
                  head_sem, w_sems, in_sems, out_sems):
    n_src, slots, sub, _ = out_ref.shape
    groups = pl.cdiv(slots, PAIR)
    core = lax.rem(lax.axis_index(AXIS), 2)
    loads = []
    for k, (up, down) in enumerate(((up_own, down_own), (up_other, down_other))):
        loads.append((pltpu.make_async_copy(up.at[0], up_ref.at[k], w_sems.at[k, 0]),
                      pltpu.make_async_copy(down.at[0], down_ref.at[k], w_sems.at[k, 1])))
    size_of = [min(PAIR, slots - g * PAIR) for g in range(groups)]

    def fetch(g, size):
        return pltpu.make_async_copy(x_ref.at[:, pl.ds(g * PAIR * sub, size * sub)], rows_ref.at[g, :, pl.ds(0, size * sub)], in_sems.at[g])

    def hand_back(g, i, size):
        return pltpu.make_async_copy(rows_ref.at[g, :, pl.ds(i * sub, sub)], out_ref.at[:, g * PAIR + i], out_sems.at[g, i])

    heads = pltpu.make_async_copy(x_ref.at[:, pl.ds(slots * sub, HEAD)], head_ref, head_sem)
    heads.start()
    for load in loads[0]:
        load.start()
    for g in range(groups):
        fetch(g, size_of[g]).start()
    for load in loads[1]:
        load.start()
    ready_ref[0] = 0
    heads.wait()
    head = head_ref[...].astype(jnp.float32)
    low, high = head[:, 0:1, :], head[:, 1:2, :]
    n_low = jnp.max(low).astype(jnp.int32)
    n_high = jnp.max(jnp.minimum(high, 2 * slots - low)).astype(jnp.int32)
    left_ref[0] = jnp.max(head[:, 2:3, :]).astype(jnp.int32)
    for load in loads[0]:
        load.wait()

    def each_size(g, act):
        @pl.when(g < groups - 1)
        def _():
            act(PAIR)

        @pl.when(g == groups - 1)
        def _():
            act(size_of[-1])

    def send_back(g, size):
        for i in range(size):
            hand_back(g, i, size).start()

    def group(step, carry):
        g = jnp.where(core == 0, step, groups - 1 - step)
        each_size(g, lambda size: fetch(g, size).wait())
        p = core * slots + g * PAIR
        has_low = p < n_low
        has_high = jnp.minimum(p + PAIR, (core + 1) * slots) > 2 * slots - n_high
        needs_other = jnp.where(core == 0, has_high, has_low)

        @pl.when(needs_other & (ready_ref[0] == 0))
        def _():
            for load in loads[1]:
                load.wait()
            ready_ref[0] = 1

        @pl.when(has_low != has_high)
        def _():
            k = needs_other.astype(jnp.int32)
            out = mlp(rows_ref[g].reshape(PAIR * n_src, -1), up_ref[k], down_ref[k])
            rows_ref[g] = out.reshape(rows_ref.shape[1:])

        @pl.when(has_low & has_high)
        def _():
            rows = rows_ref[g].reshape(PAIR * n_src, -1)
            first = mlp(rows, up_ref[core], down_ref[core]).reshape(rows_ref.shape[1:]).astype(jnp.float32)
            second = mlp(rows, up_ref[1 - core], down_ref[1 - core]).reshape(rows_ref.shape[1:]).astype(jnp.float32)
            slot = (p + lax.broadcasted_iota(jnp.int32, rows_ref.shape[1:], 1) // sub).astype(jnp.float32)
            rows_ref[g] = jnp.where(head_ref[:, 0:1, :].astype(jnp.float32) > slot, first, second).astype(jnp.bfloat16)

        each_size(g, lambda size: send_back(g, size))
        return carry

    lax.fori_loop(0, groups, group, 0)

    @pl.when(ready_ref[0] == 0)
    def _():
        for load in loads[1]:
            load.wait()

    for g in range(groups):
        for i in range(size_of[g]):
            hand_back(g, i, size_of[g]).wait()


def late_expert_kernel(x_ref, up_ref, down_ref, out_ref):
    def tile(i, carry):
        out_ref[i] = mlp(x_ref[i].reshape(x_ref.shape[1], -1), up_ref[0], down_ref[0]).reshape(x_ref.shape[1:])
        return carry

    lax.fori_loop(0, x_ref.shape[0], tile, 0)


def combine_kernel(pos_ref, gate_ref, back_ref, *refs):
    late_ref, (y_ref, acc_ref) = (refs[0] if len(refs) == 3 else None), refs[-2:]
    top_k, tok_dev = pos_ref.shape
    count = back_ref.shape[0]

    def body(t, carry):
        total = None
        for j in range(top_k):
            at = pos_ref[j, t]
            row = back_ref[jnp.minimum(at, count - 1)]
            if late_ref is not None:
                row = jnp.where(at < count, row, late_ref[jnp.maximum(at - count, 0)])
            term = gate_ref[j, t] * row.astype(jnp.float32)
            total = term if total is None else total + term
        acc_ref[t] = total.astype(jnp.bfloat16)
        return carry

    lax.fori_loop(0, tok_dev, body, 0, unroll=2)
    y_ref[...] = acc_ref[...].reshape(y_ref.shape)


def solution(mesh):
    n_dev = mesh.shape[AXIS]
    swap = [(i, i ^ 1) for i in range(n_dev)]

    def local_moe(x_loc, idx_loc, gate_loc, up_loc, down_loc):
        tok_dev, d_model = x_loc.shape
        top_k = idx_loc.shape[1]
        d_ff = up_loc.shape[2]
        sub = d_model // LANES
        count, late_count = n_dev * SLOTS, n_dev * REST
        vmem = pl.BlockSpec(memory_space=pltpu.VMEM)
        smem = pl.BlockSpec(memory_space=pltpu.SMEM)
        anywhere = pl.BlockSpec(memory_space=pl.ANY)
        tile_of = lambda n: jax.ShapeDtypeStruct((n, sub, LANES), jnp.bfloat16)
        dma = pltpu.SemaphoreType.DMA
        scratch = lambda *shape: pltpu.VMEM(shape + (sub, LANES), jnp.bfloat16)
        idx_t, gate_t = idx_loc.T, gate_loc.T
        up_other = lax.ppermute(up_loc, AXIS, swap)
        down_other = lax.ppermute(down_loc, AXIS, swap)

        def exchange(rows):
            return lax.all_to_all(rows, AXIS, 0, 0, tiled=True)

        block = SLOTS * sub + HEAD
        sent, pos = pl.pallas_call(
            pack_kernel,
            out_shape=[jax.ShapeDtypeStruct((n_dev, block, LANES), jnp.bfloat16), jax.ShapeDtypeStruct((top_k, tok_dev), jnp.int32)],
            in_specs=[vmem, vmem], out_specs=[anywhere, vmem],
            scratch_shapes=[scratch(tok_dev), pltpu.VMEM((n_dev + 1, block, LANES), jnp.bfloat16), pltpu.VMEM((top_k, tok_dev), jnp.int32),
                            pltpu.SMEM((top_k, tok_dev), jnp.int32), dma((2,))],
            name='pack')(idx_t, x_loc)
        came = exchange(sent)
        groups = -(-SLOTS // PAIR)
        done, left = pl.pallas_call(
            expert_kernel, out_shape=[jax.ShapeDtypeStruct((n_dev, SLOTS, sub, LANES), jnp.bfloat16), jax.ShapeDtypeStruct((1,), jnp.int32)],
            in_specs=[anywhere] * 5, out_specs=[anywhere, smem],
            scratch_shapes=[pltpu.VMEM((groups, n_dev, PAIR * sub, LANES), jnp.bfloat16), pltpu.VMEM((n_dev, HEAD, LANES), jnp.bfloat16),
                            pltpu.VMEM((2, d_model, d_ff), jnp.bfloat16), pltpu.VMEM((2, d_ff, d_model), jnp.bfloat16), pltpu.SMEM((1,), jnp.int32),
                            dma, dma((2, 2)), dma((groups,)), dma((groups, PAIR))],
            cost_estimate=pl.CostEstimate(flops=4 * count * d_model * d_ff, bytes_accessed=4 * count * d_model + 8 * d_model * d_ff,
                                          transcendentals=count * d_ff),
            compiler_params=pltpu.CompilerParams(vmem_limit_bytes=62 * 2**20), name='experts')(came, up_loc, down_loc, up_other, down_other)
        back = exchange(done.reshape(count, sub, LANES))

        def combine(*backs):
            return pl.pallas_call(
                combine_kernel, out_shape=jax.ShapeDtypeStruct((tok_dev, d_model), jnp.bfloat16),
                in_specs=[smem, smem] + [vmem] * len(backs), out_specs=vmem, scratch_shapes=[scratch(tok_dev)], name='combine')(pos, gate_t, *backs)

        def second_pass():
            rows = pl.pallas_call(
                pack_late_kernel, out_shape=tile_of(late_count), in_specs=[smem, vmem], out_specs=anywhere,
                scratch_shapes=[scratch(tok_dev), scratch(late_count + 8), dma((1,))], name='pack_late')(pos, x_loc)
            odd = lax.rem(lax.axis_index(AXIS), 2) == 1
            up, down = jnp.where(odd, up_loc, up_other), jnp.where(odd, down_loc, down_other)
            out = pl.pallas_call(
                late_expert_kernel, out_shape=jax.ShapeDtypeStruct((REST, n_dev, sub, LANES), jnp.bfloat16),
                in_specs=[vmem] * 3, out_specs=vmem, name='late_experts')(exchange(rows).reshape(REST, n_dev, sub, LANES), up, down)
            return combine(back, exchange(out.reshape(late_count, sub, LANES)))

        return lax.cond(left[0] == 0, lambda: combine(back), second_pass)

    tok_spec = P(('data', AXIS), None)
    w_spec = P(AXIS, None, None)
    return jax.shard_map(local_moe, mesh=mesh, in_specs=(tok_spec, tok_spec, tok_spec, w_spec, w_spec), out_specs=tok_spec, check_vma=False)
```

```python
import jax
import jax.numpy as jnp
from jax import lax
from jax.experimental import pallas as pl
from jax.experimental.pallas import tpu as pltpu
from jax.sharding import PartitionSpec as P


AXIS = 'expert'
LANES = 128
SLOT_CAP = 16
SLOTS = 11
REST = SLOT_CAP - SLOTS
PAIR = 2
HEAD = 8
STRIDE = 256


def copy_rows(rows_ref, top_k, put):
    def body(t, carry):
        row = rows_ref[t]
        for j in range(top_k):
            put(j, t, row)
        return carry

    lax.fori_loop(0, rows_ref.shape[0], body, 0, unroll=2)


def pack_kernel(idx_ref, x_ref, out_ref, pos_ref, rows_ref, blocks_ref, at_ref, at_smem, sems):
    top_k, tok_dev = idx_ref.shape
    n_exp = out_ref.shape[0]
    sub = rows_ref.shape[1]
    expert = lax.broadcasted_iota(jnp.int32, (n_exp, tok_dev), 0)
    hits = [idx_ref[j:j + 1, :] == expert for j in range(top_k)]
    chosen = sum(h.astype(jnp.float32) for h in hits)
    t_row = lax.broadcasted_iota(jnp.int32, (tok_dev, tok_dev), 0)
    t_col = lax.broadcasted_iota(jnp.int32, (tok_dev, tok_dev), 1)
    rank = jnp.dot(chosen.astype(jnp.bfloat16), (t_row < t_col).astype(jnp.bfloat16), preferred_element_type=jnp.float32)
    e_row = lax.broadcasted_iota(jnp.int32, (n_exp, n_exp), 0)
    e_col = lax.broadcasted_iota(jnp.int32, (n_exp, n_exp), 1)
    beside = ((e_col + 1 == e_row) & (lax.rem(e_row, 2) == 1)).astype(jnp.bfloat16)
    ahead = jnp.sum(jnp.dot(beside, chosen.astype(jnp.bfloat16), preferred_element_type=jnp.float32), axis=1, keepdims=True)
    odd = lax.rem(expert, 2)
    chip0 = (expert - odd).astype(jnp.float32)
    p = jnp.where(odd == 1, 2 * SLOTS - 1 - rank, rank)
    core = (p >= SLOTS).astype(jnp.float32)
    i = p - core * SLOTS
    late = ahead + rank - 2 * SLOTS
    is_late = (odd == 1) & (late >= 0)
    late_core = (late >= REST).astype(jnp.float32)
    slot = jnp.where(is_late, n_exp * SLOTS + (chip0 + late_core) * REST + late - late_core * REST, (chip0 + core) * SLOTS + i)
    at = jnp.where(is_late, float(n_exp * STRIDE), (chip0 + core) * STRIDE + i * sub)
    of_pair = lambda v: jnp.concatenate([jnp.sum(jnp.where(h, v, 0.0), axis=0, keepdims=True) for h in hits], axis=0).astype(jnp.int32)
    at_ref[...] = of_pair(at)
    to_smem = pltpu.make_async_copy(at_ref, at_smem, sems.at[0])
    to_smem.start()
    pos_ref[...] = of_pair(slot)
    total = lax.dot_general(jnp.ones((HEAD, tok_dev), jnp.bfloat16), chosen.astype(jnp.bfloat16), (((1,), (1,)), ((), ())),
                            preferred_element_type=jnp.float32)
    blocks_ref[pl.ds(0, n_exp), pl.ds(SLOTS * sub, HEAD)] = jnp.broadcast_to(total.astype(jnp.bfloat16)[None], (n_exp, HEAD, LANES))
    rows_ref[...] = x_ref[...].reshape(rows_ref.shape)
    to_smem.wait()

    def put(j, t, row):
        at = at_smem[j, t]
        blocks_ref[at // STRIDE, pl.ds(pl.multiple_of(at % STRIDE, sub), sub)] = row

    copy_rows(rows_ref, top_k, put)
    out = pltpu.make_async_copy(blocks_ref.at[pl.ds(0, n_exp)], out_ref, sems.at[1])
    out.start()
    out.wait()


def pack_late_kernel(pos_ref, x_ref, out_ref, rows_ref, slots_ref, sems):
    count = out_ref.shape[0]
    rows_ref[...] = x_ref[...].reshape(rows_ref.shape)

    def put(j, t, row):
        at = pos_ref[j, t] - count // REST * SLOTS
        slots_ref[jnp.where(at < 0, count, at)] = row

    copy_rows(rows_ref, pos_ref.shape[0], put)
    out = pltpu.make_async_copy(slots_ref.at[pl.ds(0, count)], out_ref, sems.at[0])
    out.start()
    out.wait()


def mlp(rows, up, down):
    hidden = jnp.dot(rows, up, preferred_element_type=jnp.float32)
    hidden = jax.nn.gelu(hidden, approximate=True).astype(jnp.bfloat16)
    return jnp.dot(hidden, down, preferred_element_type=jnp.float32).astype(jnp.bfloat16)


def expert_kernel(x_ref, up_own, down_own, up_other, down_other, out_ref, left_ref, rows_ref, head_ref, up_ref, down_ref, low_ref, ready_ref,
                  head_sem, w_sems, in_sems, out_sems):
    n_src, slots, sub, _ = out_ref.shape
    groups = pl.cdiv(slots, PAIR)
    core = lax.rem(lax.axis_index(AXIS), 2)
    loads = []
    for k, (up, down) in enumerate(((up_own, down_own), (up_other, down_other))):
        loads.append((pltpu.make_async_copy(up.at[0], up_ref.at[k], w_sems.at[k, 0]),
                      pltpu.make_async_copy(down.at[0], down_ref.at[k], w_sems.at[k, 1])))
    size_of = [min(PAIR, slots - g * PAIR) for g in range(groups)]

    def fetch(g, size):
        return pltpu.make_async_copy(x_ref.at[:, pl.ds(g * PAIR * sub, size * sub)], rows_ref.at[g, :, pl.ds(0, size * sub)], in_sems.at[g])

    def hand_back(g, i):
        return pltpu.make_async_copy(rows_ref.at[g, :, pl.ds(i * sub, sub)], out_ref.at[:, g * PAIR + i], out_sems.at[g, i])

    heads = pltpu.make_async_copy(x_ref.at[:, pl.ds(slots * sub, HEAD)], head_ref, head_sem)

    def each_size(g, act):
        @pl.when(g < groups - 1)
        def _():
            act(PAIR)

        @pl.when(g == groups - 1)
        def _():
            act(size_of[-1])

    def order(step):
        return jnp.where(core == 0, step, groups - 1 - step)

    heads.start()
    for load in loads[0]:
        load.start()
    each_size(order(0), lambda size: fetch(order(0), size).start())
    ready_ref[0] = 0
    heads.wait()
    counts = head_ref[:, 0, :].astype(jnp.float32)
    row = lax.broadcasted_iota(jnp.int32, (n_src, n_src), 0)
    lane = lax.broadcasted_iota(jnp.int32, (n_src, n_src), 1)
    chip = lax.axis_index(AXIS) - core
    low = jnp.sum(jnp.where(lane == chip, counts, 0.0), axis=1, keepdims=True)
    high = jnp.sum(jnp.where(lane == chip + 1, counts, 0.0), axis=1, keepdims=True)
    low_ref[...] = jnp.broadcast_to(low[:, :, None], low_ref.shape)
    pooled = jnp.dot(counts.astype(jnp.bfloat16), (row // 2 == lane // 2).astype(jnp.bfloat16), preferred_element_type=jnp.float32)
    n_low = jnp.max(low).astype(jnp.int32)
    n_high = jnp.max(jnp.minimum(high, 2 * slots - low)).astype(jnp.int32)
    left_ref[0] = (jnp.max(pooled) > 2 * slots).astype(jnp.int32)
    for load in loads[0]:
        load.wait()
    for step in range(1, groups):
        each_size(order(step), lambda size: fetch(order(step), size).start())
    for load in loads[1]:
        load.start()

    def send_back(g, size):
        for i in range(size):
            hand_back(g, i).start()

    def group(step, carry):
        g = order(step)
        each_size(g, lambda size: fetch(g, size).wait())
        p = core * slots + g * PAIR
        has_low = p < n_low
        has_high = jnp.minimum(p + PAIR, (core + 1) * slots) > 2 * slots - n_high
        needs_other = jnp.where(core == 0, has_high, has_low)

        @pl.when(needs_other & (ready_ref[0] == 0))
        def _():
            for load in loads[1]:
                load.wait()
            ready_ref[0] = 1

        @pl.when(has_low != has_high)
        def _():
            k = needs_other.astype(jnp.int32)
            out = mlp(rows_ref[g].reshape(PAIR * n_src, -1), up_ref[k], down_ref[k])
            rows_ref[g] = out.reshape(rows_ref.shape[1:])

        @pl.when(has_low & has_high)
        def _():
            rows = rows_ref[g].reshape(PAIR * n_src, -1)
            first = mlp(rows, up_ref[core], down_ref[core]).reshape(rows_ref.shape[1:]).astype(jnp.float32)
            second = mlp(rows, up_ref[1 - core], down_ref[1 - core]).reshape(rows_ref.shape[1:]).astype(jnp.float32)
            slot = (p + lax.broadcasted_iota(jnp.int32, rows_ref.shape[1:], 1) // sub).astype(jnp.float32)
            rows_ref[g] = jnp.where(low_ref[...] > slot, first, second).astype(jnp.bfloat16)

        each_size(g, lambda size: send_back(g, size))
        return carry

    lax.fori_loop(0, groups, group, 0)

    @pl.when(ready_ref[0] == 0)
    def _():
        for load in loads[1]:
            load.wait()

    for g in range(groups):
        for i in range(size_of[g]):
            hand_back(g, i).wait()


def late_expert_kernel(x_ref, up_ref, down_ref, out_ref):
    def tile(i, carry):
        out_ref[i] = mlp(x_ref[i].reshape(x_ref.shape[1], -1), up_ref[0], down_ref[0]).reshape(x_ref.shape[1:])
        return carry

    lax.fori_loop(0, x_ref.shape[0], tile, 0)


def combine_kernel(pos_ref, gate_ref, back_ref, *refs):
    late_ref, (y_ref, acc_ref) = (refs[0] if len(refs) == 3 else None), refs[-2:]
    top_k, tok_dev = pos_ref.shape
    count = back_ref.shape[0]

    def body(t, carry):
        total = None
        for j in range(top_k):
            at = pos_ref[j, t]
            row = back_ref[jnp.minimum(at, count - 1)]
            if late_ref is not None:
                row = jnp.where(at < count, row, late_ref[jnp.maximum(at - count, 0)])
            term = gate_ref[j, t] * row.astype(jnp.float32)
            total = term if total is None else total + term
        acc_ref[t] = total.astype(jnp.bfloat16)
        return carry

    lax.fori_loop(0, tok_dev, body, 0, unroll=2)
    y_ref[...] = acc_ref[...].reshape(y_ref.shape)


def solution(mesh):
    n_dev = mesh.shape[AXIS]
    swap = [(i, i ^ 1) for i in range(n_dev)]

    def local_moe(x_loc, idx_loc, gate_loc, up_loc, down_loc):
        tok_dev, d_model = x_loc.shape
        top_k = idx_loc.shape[1]
        d_ff = up_loc.shape[2]
        sub = d_model // LANES
        count, late_count = n_dev * SLOTS, n_dev * REST
        vmem = pl.BlockSpec(memory_space=pltpu.VMEM)
        smem = pl.BlockSpec(memory_space=pltpu.SMEM)
        anywhere = pl.BlockSpec(memory_space=pl.ANY)
        tile_of = lambda n: jax.ShapeDtypeStruct((n, sub, LANES), jnp.bfloat16)
        dma = pltpu.SemaphoreType.DMA
        scratch = lambda *shape: pltpu.VMEM(shape + (sub, LANES), jnp.bfloat16)
        idx_t, gate_t = idx_loc.T, gate_loc.T
        up_other = lax.ppermute(up_loc, AXIS, swap)
        down_other = lax.ppermute(down_loc, AXIS, swap)

        def exchange(rows):
            return lax.all_to_all(rows, AXIS, 0, 0, tiled=True)

        block = SLOTS * sub + HEAD
        sent, pos = pl.pallas_call(
            pack_kernel,
            out_shape=[jax.ShapeDtypeStruct((n_dev, block, LANES), jnp.bfloat16), jax.ShapeDtypeStruct((top_k, tok_dev), jnp.int32)],
            in_specs=[vmem, vmem], out_specs=[anywhere, vmem],
            scratch_shapes=[scratch(tok_dev), pltpu.VMEM((n_dev + 1, block, LANES), jnp.bfloat16), pltpu.VMEM((top_k, tok_dev), jnp.int32),
                            pltpu.SMEM((top_k, tok_dev), jnp.int32), dma((2,))],
            name='pack')(idx_t, x_loc)
        came = exchange(sent)
        groups = -(-SLOTS // PAIR)
        done, left = pl.pallas_call(
            expert_kernel, out_shape=[jax.ShapeDtypeStruct((n_dev, SLOTS, sub, LANES), jnp.bfloat16), jax.ShapeDtypeStruct((1,), jnp.int32)],
            in_specs=[anywhere] * 5, out_specs=[anywhere, smem],
            scratch_shapes=[pltpu.VMEM((groups, n_dev, PAIR * sub, LANES), jnp.bfloat16), pltpu.VMEM((n_dev, HEAD, LANES), jnp.bfloat16),
                            pltpu.VMEM((2, d_model, d_ff), jnp.bfloat16), pltpu.VMEM((2, d_ff, d_model), jnp.bfloat16), pltpu.VMEM((n_dev, 1, LANES), jnp.float32), pltpu.SMEM((1,), jnp.int32),
                            dma, dma((2, 2)), dma((groups,)), dma((groups, PAIR))],
            cost_estimate=pl.CostEstimate(flops=4 * count * d_model * d_ff, bytes_accessed=4 * count * d_model + 8 * d_model * d_ff,
                                          transcendentals=count * d_ff),
            compiler_params=pltpu.CompilerParams(vmem_limit_bytes=62 * 2**20), name='experts')(came, up_loc, down_loc, up_other, down_other)
        back = exchange(done.reshape(count, sub, LANES))

        def combine(*backs):
            return pl.pallas_call(
                combine_kernel, out_shape=jax.ShapeDtypeStruct((tok_dev, d_model), jnp.bfloat16),
                in_specs=[smem, smem] + [vmem] * len(backs), out_specs=vmem, scratch_shapes=[scratch(tok_dev)], name='combine')(pos, gate_t, *backs)

        def second_pass():
            rows = pl.pallas_call(
                pack_late_kernel, out_shape=tile_of(late_count), in_specs=[smem, vmem], out_specs=anywhere,
                scratch_shapes=[scratch(tok_dev), scratch(late_count + 8), dma((1,))], name='pack_late')(pos, x_loc)
            odd = lax.rem(lax.axis_index(AXIS), 2) == 1
            up, down = jnp.where(odd, up_loc, up_other), jnp.where(odd, down_loc, down_other)
            out = pl.pallas_call(
                late_expert_kernel, out_shape=jax.ShapeDtypeStruct((REST, n_dev, sub, LANES), jnp.bfloat16),
                in_specs=[vmem] * 3, out_specs=vmem, name='late_experts')(exchange(rows).reshape(REST, n_dev, sub, LANES), up, down)
            return combine(back, exchange(out.reshape(late_count, sub, LANES)))

        return lax.cond(left[0] == 0, lambda: combine(back), second_pass)

    tok_spec = P(('data', AXIS), None)
    w_spec = P(AXIS, None, None)
    return jax.shard_map(local_moe, mesh=mesh, in_specs=(tok_spec, tok_spec, tok_spec, w_spec, w_spec), out_specs=tok_spec, check_vma=False)
```
